32 devices in a mesh: prow: 16 (over z, y, core), pcol: 2 (over x).
Axes of the slice: x: 2, y: 2, z: 4, core: 2. Of those that a mesh axis runs over, the one named last changes fastest.
Arguments:
- factor_panel: float32 [2048, 31744], P('pcol', 'prow'), may hold values from -0.03125 to 0.03125
- whitened_before: float32 [31744, 4096], P('prow', 'pcol'), may hold values from -6 to 6
- green_panel: float32 [2048, 4096], P('prow', 'pcol'), may hold values from -6 to 6
- diag_inverse: float32 [2048, 2048], P('prow', 'pcol'), may hold values from -1 to 8, as said below
Outputs:
- whitened: float32 [2048, 4096], P('prow', 'pcol')
- gram_block: float32 [4096, 4096], P('prow', 'pcol')
The draws below stay inside these ranges and needn't reach their ends.
Inputs may be any that keep to these rules, and one draw needn't show every extreme that they name: `diag_inverse`: zero above the diagonal and positive on it.
All inputs are finite; a program needn't handle non-finite values.
Results may differ from the reference program's by a relative error of at most 0.00012.
Values sent between devices are 32-bit elements; how exact they have to be, the bound alone decides.
No kernel may reach another device: no remote copies, remote signals or barrier semaphores. Data moves between devices by JAX's collectives and lax.ppermute only.
A program may use at most 128 MiB of HBM per device.

```python
import math
import jax
import jax.numpy as jnp
from jax import lax

P_SIZE = 4096
B = 2048
K = 31744


def draw_diag_inverse(key, part):
    first_key, second_key = jax.random.split(jax.random.fold_in(key, 7), 2)
    lower = jax.random.normal(first_key, (B, B), jnp.float32) * (0.7 / math.sqrt(B))
    diagonal = jnp.exp(jax.random.uniform(second_key, (B,), jnp.float32, math.log(0.5), math.log(2.0)))
    matrix = jnp.tril(lower, -1) + jnp.diag(diagonal)
    return matrix


def block_scale(rng, dims, cuts, low, high):
    def one(position, shards_of):
        steps = jax.random.uniform(jax.random.fold_in(jax.random.fold_in(rng, 6), position), (shards_of,), jnp.float32, low / len(cuts), high / len(cuts))
        return jnp.repeat(jnp.exp(steps), dims[position] // shards_of).reshape((-1,) + (1,) * (len(dims) - position - 1))

    gain = one(*cuts[0])
    for cut in cuts[1:]:
        gain = gain * one(*cut)
    return gain


def scatter_about(own_key, extent, spread, reach, pieces=(), dtype=jnp.bfloat16):
    entries = spread * jax.random.normal(own_key, extent, jnp.float32)
    if pieces:
        entries = entries * block_scale(own_key, extent, pieces, -0.22, 0.18)
    return jnp.clip(entries, -reach, reach).astype(dtype)


def setup_inputs(seed: int = 0) -> dict:
    streams_of = jax.random.split(jax.random.key(seed), 5)
    factor_panel = scatter_about(streams_of[0], (B, K), K ** -0.5, 0.03125, ((0, 2), (1, 16)), jnp.float32)
    whitened_before = scatter_about(streams_of[1], (K, P_SIZE), 1.0, 6.0, ((0, 16), (1, 2)), jnp.float32)
    green_panel = scatter_about(streams_of[2], (B, P_SIZE), 1.0, 6.0, ((0, 16), (1, 2)), jnp.float32)
    diag_inverse = draw_diag_inverse(jax.random.fold_in(streams_of[4], 71), 0)
    return {"factor_panel": factor_panel, "whitened_before": whitened_before, "green_panel": green_panel, "diag_inverse": diag_inverse}


def reference(factor_panel, whitened_before, green_panel, diag_inverse):
    highest = lax.Precision.HIGHEST
    remaining = green_panel - jnp.dot(factor_panel, whitened_before, precision=highest, preferred_element_type=jnp.float32)
    whitened = jnp.dot(diag_inverse, remaining, precision=highest, preferred_element_type=jnp.float32)
    gram_block = jnp.dot(whitened.T, whitened, precision=highest, preferred_element_type=jnp.float32) * (1.0 / B)
    return whitened, gram_block
```

```python
import jax
import jax.numpy as jnp
from jax import lax
from jax.sharding import PartitionSpec as P


OWN_PARTS = (1, 3)
RECV_PARTS = (3, 3, 2)
TAIL_PARTS = (1, 1)

high = lax.Precision.HIGH


def mm(a, b):
    return jnp.dot(a, b, precision=high, preferred_element_type=jnp.float32)


def mm_t(a, b):
    return lax.dot_general(a, b, (((0,), (0,)), ((), ())), precision=high, preferred_element_type=jnp.float32)


def spans(parts, total):
    unit = total // sum(parts)
    out, at = [], 0
    for p in parts:
        out.append((at, at + p * unit))
        at += p * unit
    return out


def gather_rows(value, r, bits, size):
    done = []
    for bit in bits:
        got = lax.ppermute(value, "prow", [(i, i ^ bit) for i in range(size)])
        mine = (r & bit) != 0
        axis = sum(1 for b in done if b > bit)
        value = jnp.stack([jnp.where(mine, got, value), jnp.where(mine, value, got)], axis=axis)
        done.append(bit)
    return value.reshape((-1, value.shape[-1]))


def bit_list(size):
    return [1 << k for k in range(size.bit_length() - 1)]


def swap(value, bit, size):
    return lax.ppermute(value, "prow", [(i, i ^ bit) for i in range(size)])


def scatter_columns(value, r, size):
    for bit in bit_list(size):
        w = value.shape[1] // 2
        mine = (r & bit) != 0
        left, right = value[:, :w], value[:, w:]
        got = swap(jnp.where(mine, left, right), bit, size)
        value = jnp.where(mine, right, left) + got
    return value


def gather_columns(value, r, size):
    held = None
    for bit in reversed(bit_list(size)):
        got = swap(value, bit, size)
        if bit == 1:
            return held, value, got
        mine = (r & bit) != 0
        value = jnp.concatenate([jnp.where(mine, got, value), jnp.where(mine, value, got)], axis=1)
        held = value if held is None else held


def column_slot(r, size):
    n = len(bit_list(size))
    return sum(((r >> k) & 1) << (n - 1 - k) for k in range(n))


def pair_shards(factor, before, green, dinv):
    size = lax.axis_size("prow")
    r = lax.axis_index("prow")
    c = lax.axis_index("pcol")
    first = c == 0
    half, rows_g = factor.shape[0], green.shape[0]
    width = before.shape[1]
    panel = 2 * half
    top = size // 2
    cross = [(0, 1), (1, 0)]
    own_spans = spans(OWN_PARTS, half)
    recv_spans = spans(RECV_PARTS, half)

    came = []
    for lo, hi in recv_spans:
        came.append(lax.ppermute(factor[lo:hi], "pcol", cross))

    def reduced(rows, base):
        n = rows.shape[0] // rows_g
        prod, placed = lax.optimization_barrier((mm(rows, before), green))
        prod = prod.reshape(n, rows_g, width)
        here = (base // rows_g + lax.broadcasted_iota(jnp.int32, (n, 1, 1), 0)) == r
        part = (jnp.where(here, placed[None], 0.0) - prod).reshape(n * rows_g, width)
        return scatter_columns(part, r, size)

    rem_own = jnp.concatenate([reduced(factor[lo:hi], c * half + lo) for lo, hi in own_spans], axis=0)

    other = lax.ppermute(dinv, "pcol", cross)
    dleft = jnp.where(first, dinv, other)
    dright = jnp.where(first, other, dinv)
    bits = bit_list(size)
    got = lax.ppermute(dright, "prow", [(i, i - top) for i in range(top, size)])
    dright = jnp.where(r >= top, dright, got)
    dleft = gather_rows(dleft, r, bits[::-1], size)
    dright = gather_rows(dright, r, bits[1:-1] + bits[:1], size)

    pairs = []
    for cn in (0, 1):
        for i in range(cn * top, (cn + 1) * top):
            pairs.append((i * 2 + cn, (cn * top + column_slot(i, size) // 2) * 2 + 1 - cn))

    def finish(x):
        held, kept, got = gather_columns(x, r, size)
        crossed = lax.ppermute(held, ("prow", "pcol"), pairs)
        return kept, got, crossed

    rem_recv, recv_done = [], []
    for rows, (lo, hi) in zip(came, recv_spans):
        rem_recv.append(reduced(rows, (1 - c) * half + lo))
        known = jnp.concatenate(rem_recv, axis=0)
        by_own = jnp.where(first, dleft[half + lo:half + hi], 0.0)
        by_recv = jnp.where(first, dright[lo:hi, :hi], dleft[lo:hi, :hi])
        x = mm(by_own, rem_own) + mm(by_recv, known)
        recv_done.append(finish(x))
    by_own = jnp.where(first, dleft[:half], dright)
    by_recv = jnp.where(first, 0.0, dleft[half:])
    x_own = mm(by_own, rem_own) + mm(by_recv, known)
    cut = lax.optimization_barrier([x_own[lo:hi] for lo, hi in spans(TAIL_PARTS, half)])
    own_done = [finish(x) for x in cut]
    cross_recv = jnp.concatenate([v[2] for v in recv_done], axis=0)
    cross_own = jnp.concatenate([v[2] for v in own_done], axis=0)

    sub = 2 * width // size
    wide = width // 2
    upper = (r >= top) == (c == 1)
    odd = (r & 1) != 0
    start = (r % top) * sub
    in_kept = (start >= wide) == odd
    at = (r % top) * rows_g
    grams = [jnp.zeros((sub, wide), jnp.float32)] * 2
    rows_kept, rows_got = jnp.zeros((rows_g, wide), jnp.float32), jnp.zeros((rows_g, wide), jnp.float32)
    groups = [(recv_done, recv_spans, cross_own, ~upper), (own_done, spans(TAIL_PARTS, half), cross_recv, upper)]
    for done, cuts, cross_all, holds in groups:
        for (kept, got, _), (lo, hi) in zip(done, cuts):
            pieces = [lax.dynamic_slice_in_dim(v, start % wide, sub, 1) for v in (kept, got)]
            needed = jnp.where(upper, jnp.where(in_kept, *pieces), cross_all[lo:hi])
            grams = [g + mm_t(needed, v) for g, v in zip(grams, (kept, got))]
            hit = holds & (at >= lo) & (at < hi)
            spot = jnp.clip(at - lo, 0, hi - lo - rows_g)
            rows_kept = jnp.where(hit, lax.dynamic_slice_in_dim(kept, spot, rows_g, 0), rows_kept)
            rows_got = jnp.where(hit, lax.dynamic_slice_in_dim(got, spot, rows_g, 0), rows_got)

    def ordered(kept, got):
        return jnp.concatenate([jnp.where(odd, got, kept), jnp.where(odd, kept, got)], axis=1)

    return ordered(rows_kept, rows_got), ordered(*grams) * (1.0 / panel)


def many_shards(factor, before, green, dinv):
    rows_all = lax.all_gather(factor, "pcol", axis=0, tiled=True)
    update = lax.psum_scatter(mm(rows_all, before), "prow", scatter_dimension=0, tiled=True)
    remaining = lax.all_gather(green - update, "prow", axis=0, tiled=True)
    whitened = mm(lax.all_gather(dinv, "pcol", axis=1, tiled=True), remaining)
    column_all = lax.all_gather(whitened, "prow", axis=0, tiled=True)
    rows, cols = lax.axis_size("prow"), lax.axis_size("pcol")
    local_width = before.shape[1]
    sub_width = local_width * cols // rows
    row = lax.axis_index("prow")
    own = lax.dynamic_slice_in_dim(column_all, row * sub_width % local_width, sub_width, 1)
    kept = jnp.where(lax.axis_index("pcol") == row * cols // rows, own, 0.0)
    gram = mm_t(lax.psum(kept, "pcol"), column_all) * (1.0 / column_all.shape[0])
    return whitened, gram


def solution(mesh):
    rows, cols = mesh.shape["prow"], mesh.shape["pcol"]
    paired = cols == 2 and rows & (rows - 1) == 0 and rows == 16

    def body(*args):
        if not paired:
            return many_shards(*args)
        return pair_shards(*args)

    return jax.shard_map(
        body,
        mesh=mesh,
        in_specs=(P("pcol", "prow"), P("prow", "pcol"), P("prow", "pcol"), P("prow", "pcol")),
        out_specs=(P("prow", "pcol"), P("prow", "pcol")),
        check_vma=False,
    )
```
